32 devices in a mesh: dp: 16 (over z, y, core), mp: 2 (over x).
Axes of the slice: x: 2, y: 2, z: 4, core: 2. Of those that a mesh axis runs over, the one named last changes fastest.
Arguments:
- inputs: bfloat16 [4, 4096, 4096], P(None, 'dp'), may hold values from -60 to 60
- gate_cotangent: bfloat16 [4, 4096, 6144], P(None, 'dp', 'mp'), may hold values from -6 to 6
- ff_blocks: int32 [4], replicated, may hold values from 24 to 48, as said below
- layer_active: int32 [4], replicated, may hold values from 0 to 1, as said below
- param: float32 [4096, 6144], P(('dp', 'mp')), may hold values from -0.09375 to 0.09375
- moment: float32 [4096, 6144], P(('dp', 'mp')), may hold values from -3 to 3
- second_moment: float32 [4096, 6144], P(('dp', 'mp')), may hold values from 0.5 to 2
Outputs:
- new_param: float32 [4096, 6144], P(('dp', 'mp'))
- new_moment: float32 [4096, 6144], P(('dp', 'mp'))
- new_second: float32 [4096, 6144], P(('dp', 'mp'))
The draws below stay inside these ranges and needn't reach their ends.
Inputs may be any that keep to these rules, and one draw needn't show every extreme that they name: `ff_blocks`: entry 0 is 6144 // 128 (the largest subnet), entry 1 is 6144 // (256) (the smallest). `layer_active`: entry 0 is 1, and exactly one of entries 1, 2 and 3 is 0.
All inputs are finite; a program needn't handle non-finite values.
Results may differ from the reference program's by a relative error of at most 0.0003.
Values sent between devices are 32-bit elements; how exact they have to be, the bound alone decides.
A program may use at most 128 MiB of HBM per device.

```python
import math
import jax
import jax.numpy as jnp
from jax import lax

D = 4096
FF = 6144
BLOCK = 128
SUBNETS = 4
STEP = 10
TOK_DEV = 256
TOKENS = 4096


def draw_inputs(key, part):
    base = jnp.clip(jax.random.normal(jax.random.fold_in(key, 5), (SUBNETS, TOKENS, D), jnp.float32), -4.0, 4.0)
    column = lax.broadcasted_iota(jnp.int32, (D,), 0)
    place = column.astype(jnp.float32) / D
    scale = 1.0 + 2.0 * place
    replicas = TOKENS // TOK_DEV
    order = jax.random.permutation(jax.random.fold_in(key, 7), replicas).astype(jnp.int32)
    owner = lax.broadcasted_iota(jnp.int32, (TOKENS,), 0) // TOK_DEV
    paired = order[owner]
    column_block = column // (D // replicas)
    boost = jnp.where(column_block[None, :] == paired[:, None], 3.0, 1.0)
    return (base * scale[None, None, :] * boost[None, :, :]).astype(jnp.bfloat16)


def draw_ff_blocks(key, part):
    most = FF // BLOCK
    half = most // 2
    first = jax.random.randint(jax.random.fold_in(key, 11), (1,), half, most + 1)
    second = jax.random.randint(jax.random.fold_in(key, 13), (1,), half, most + 1)
    head = jnp.array([most, half], jnp.int32)
    return jnp.concatenate([head, first.astype(jnp.int32), second.astype(jnp.int32), jnp.full((SUBNETS - 4,), most, jnp.int32)]).astype(jnp.int32)


def draw_layer_active(key, part):
    pick = jax.random.randint(jax.random.fold_in(key, 23), (), 1, 4)
    index = lax.broadcasted_iota(jnp.int32, (SUBNETS,), 0)
    return jnp.where(index == pick, 0, 1).astype(jnp.int32)


def block_scale(stream_key, dims, shards, smallest, high):
    gain, own = 1.0, jax.random.fold_in(stream_key, 6)
    for dim, parts in shards:
        draws = jnp.exp(jax.random.uniform(jax.random.fold_in(own, dim), (parts,), jnp.float32, smallest / len(shards), high / len(shards)))
        gain = gain * jnp.repeat(draws, dims[dim] // parts).reshape([-1 if axis == dim else 1 for axis in range(len(dims))])
    return gain


def normal_values(rng, shape, width, limit, shards=(), held_as=jnp.bfloat16):
    values = width * jax.random.normal(rng, shape, jnp.float32)
    if shards:
        values = values * block_scale(rng, shape, shards, -0.22, 0.18)
    return jnp.clip(values, -limit, limit).astype(held_as)


def setup_inputs(seed: int = 0) -> dict:
    key_list = jax.random.split(jax.random.key(seed), 8)
    return {
        "inputs": draw_inputs(jax.random.fold_in(key_list[7], 71), 0),
        "gate_cotangent": normal_values(key_list[1], (SUBNETS, TOKENS, FF), 1.0, 6.0, ((1, 16), (2, 2))),
        "ff_blocks": draw_ff_blocks(jax.random.fold_in(key_list[7], 71), 0),
        "layer_active": draw_layer_active(jax.random.fold_in(key_list[7], 71), 0),
        "param": normal_values(key_list[4], (D, FF), D ** -0.5, 0.09375, ((0, 32),), jnp.float32),
        "moment": normal_values(key_list[5], (D, FF), 0.5, 3.0, ((0, 32),), jnp.float32),
        "second_moment": jnp.clip(jnp.exp(math.log(2.0) - 1.3862944 * jax.random.uniform(key_list[6], (D, FF), jnp.float32) ** block_scale(key_list[6], (D, FF), ((0, 32),), -0.2, 0.2)), 0.5, 2.0),
    }


def reference(inputs, gate_cotangent, ff_blocks, layer_active, param, moment, second_moment):
    column = lax.broadcasted_iota(jnp.int32, (SUBNETS, FF), 1)
    keep = (column < BLOCK * ff_blocks[:, None]) & (layer_active[:, None] == 1)
    masked = jnp.where(keep[:, None, :], gate_cotangent, jnp.zeros((), jnp.bfloat16))
    rows_in = inputs.reshape(SUBNETS * TOKENS, D)
    rows_ct = masked.reshape(SUBNETS * TOKENS, FF)
    gradient = lax.dot_general(rows_in, rows_ct, (((0,), (0,)), ((), ())), preferred_element_type=jnp.float32)
    total = jnp.sqrt(jnp.sum(gradient * gradient))
    factor = jnp.minimum(1.0, jnp.sqrt(1.0 * D * FF) / (total + 1e-06))
    clipped = gradient * factor
    new_moment = 0.9 * moment + 0.1 * clipped
    new_second = 0.95 * second_moment + 0.05 * clipped * clipped
    first_hat = new_moment / (1.0 - 0.9 ** STEP)
    second_hat = new_second / (1.0 - 0.95 ** STEP)
    new_param = param - 0.02 * (first_hat / (jnp.sqrt(second_hat) + 1e-08) + 0.1 * param)
    return (new_param, new_moment, new_second)
```

```python
import functools
import math

import jax
import jax.numpy as jnp
from jax import lax
from jax.experimental import pallas as pl
from jax.experimental.pallas import tpu as pltpu
from jax.sharding import PartitionSpec as P

BLOCK = 128
STEP = 10
MESH = pl.DeviceIdType.MESH
RING = 6


class Plan:
    def __init__(self, replicas, owners, width, local_cols, tokens):
        self.replicas, self.owners, self.tokens = replicas, owners, tokens
        self.line = line = replicas // 4
        self.rows = width // replicas
        self.part = self.rows // owners
        self.width, self.cols = width, local_cols
        self.wide = wide = 256 if local_cols % 512 == 0 else 128
        self.chunks = chunks = local_cols // wide
        self.half = half = chunks // 2
        self.crossings = line * chunks - half
        self.lag = 0
        while not self.fits():
            self.lag += 1
            assert self.lag < 1000
        self.ticks = self.last + chunks

    def fits(self):
        line, chunks, half = self.line, self.chunks, self.half
        self.last = (line - 1) * chunks - half + 4 + self.lag
        self.order = []
        good = True
        for at in range(line // 2):
            need = []
            for k in range(line):
                for h in range(2):
                    if (k, h) != (at ^ 1, 0):
                        need.append((self.tick_of(at, k, h * half), k, h))
            self.order.append([(k, h) for _, k, h in sorted(need)])
            for p, (k, h) in enumerate(self.order[-1]):
                for i in range(half):
                    good &= p * half + i <= self.tick_of(at, k, h * half + i)
                    good &= k != at or h == 1 or p * half + i > i
            good &= at == 0 or self.tick_of(at, at + 1, chunks - 1) < self.last
            good &= at == 0 or self.tick_of(at, at - 1, chunks - 1) < self.last
        return good

    def start(self, distance):
        return self.lag + (self.half + 2 + 2 * distance if distance else 4)

    def tick_of(self, at, k, j):
        if k == at:
            return self.last + j
        if k > at:
            return self.start(at) + (self.line - 1 - k) * self.chunks + j
        return self.start(self.line - 1 - at) + k * self.chunks + j


def pick(table, at, p):
    value = jnp.int32(0)
    for a, row in enumerate(table):
        for q, entry in enumerate(row):
            if entry:
                value = jnp.where((at == a) & (p == q), jnp.int32(entry), value)
    return value


def kernel(plan, ff, active, x_hbm, c_hbm, g_hbm, total_ref, x, c, xt, w, yr, z, dr, ds, sb, rb, ob, g, sq, parts,
           load_sem, d2d_send, d2d_recv, y_send, y_recv, z_send, z_recv, d_send, d_recv, x_send, x_recv, out_sem,
           p_send, p_recv):
    line, chunks, half, rows, wide = plan.line, plan.chunks, plan.half, plan.rows, plan.wide
    owners, part = plan.owners, plan.part
    dp, mp = lax.axis_index("dp"), lax.axis_index("mp")
    devices = plan.replicas * owners
    me = dp * owners + mp
    place, lane, core = dp // 4, (dp // 2) % 2, dp % 2
    other_core, other_lane = dp + 1 - 2 * core, dp + 2 - 4 * lane
    beside = place + 1 - 2 * (place % 2)
    far = place >= line // 2
    at = jnp.where(far, line - 1 - place, place)

    def mirrored(k):
        return jnp.where(far, line - 1 - k, k)

    loads = [
        pltpu.make_async_copy(c_hbm, c, load_sem.at[0]),
        pltpu.make_async_copy(x_hbm, x, load_sem.at[1]),
    ]
    for load in loads:
        load.start()
    barrier = pltpu.get_barrier_semaphore()

    @pl.loop(1, devices)
    def _(o):
        other = lax.rem(me + o, devices)
        pl.semaphore_signal(barrier, inc=1, device_id=(other // owners, other % owners), device_id_type=MESH)

    loads[0].wait()
    first_block = mp * (plan.cols // BLOCK)
    subnets = ff.shape[0]
    tokens = plan.tokens // subnets

    @pl.loop(0, plan.cols // BLOCK)
    def _(b):
        cols = pl.ds(pl.multiple_of(b * BLOCK, BLOCK), BLOCK)
        for s in range(subnets):
            keep = (first_block + b < ff[s]) & (active[s] == 1)
            spot = (pl.ds(s * tokens, tokens), cols)
            c[spot] = jnp.where(keep, c[spot], jnp.zeros((), c.dtype))

    sq[...] = jnp.zeros_like(sq)
    loads[1].wait()
    pl.semaphore_wait(barrier, devices - 1)

    def core_copy(q, parity):
        return pltpu.make_async_remote_copy(
            sb.at[q], rb.at[parity, q], d2d_send.at[q], d2d_recv.at[parity, q], device_id=(other_core, mp), device_id_type=MESH
        )

    def y_copy(slot, idx):
        return pltpu.make_async_remote_copy(
            w.at[slot], yr.at[idx], y_send.at[slot], y_recv.at[idx], device_id=(other_lane, mp), device_id_type=MESH
        )

    def d_copy(j):
        return pltpu.make_async_remote_copy(
            ds.at[j], dr.at[j], d_send.at[j], d_recv.at[j], device_id=(dp + 4 * (beside - place), mp), device_id_type=MESH
        )

    def z_copy(idx, slot, to):
        return pltpu.make_async_remote_copy(
            yr.at[idx], z.at[slot], z_send.at[idx], z_recv.at[slot], device_id=(dp + 4 * (to - place), mp), device_id_type=MESH
        )

    def x_copy(o, j):
        to = lax.rem(mp + o, owners)
        spot = yr.at[place * chunks + j, pl.ds(pl.multiple_of(to * part, part), part)]
        return pltpu.make_async_remote_copy(
            spot, g.at[mp * chunks + j], x_send.at[(o - 1) * chunks + j], x_recv.at[mp * chunks + j],
            device_id=(dp, to), device_id_type=MESH,
        )

    def part_copy(o):
        other = lax.rem(me + o, devices)
        return pltpu.make_async_remote_copy(
            parts.at[0], parts.at[devices - o], p_send, p_recv, device_id=(other // owners, other % owners), device_id_type=MESH
        )

    def out_copy(i):
        return pltpu.make_async_copy(
            g.at[i], g_hbm.at[:, pl.ds(pl.multiple_of(i * wide, wide), wide)], out_sem.at[i]
        )

    def produce(q, on, k, to_lane, j, fresh, parity):
        @pl.when(on)
        def _():
            @pl.when(fresh)
            def _():
                for side, owner in enumerate((1 - core, core)):
                    first = pl.multiple_of(((k * 2 + to_lane) * 2 + owner) * rows, rows)
                    xt[q, side] = x[:, pl.ds(first, rows)].T

            cols = pl.ds(pl.multiple_of(j * wide, wide), wide)
            sb[q] = jnp.dot(xt[q, 0], c[:, cols], preferred_element_type=jnp.float32)
            ob[q] = jnp.dot(xt[q, 1], c[:, cols], preferred_element_type=jnp.float32)
            core_copy(q, parity).start()

    def own(q, on, k, j, parity):
        idx = k * chunks + j

        @pl.when(on)
        def _():
            core_copy(q, parity).wait()
            crossed = (k != beside) | (j >= half)

            @pl.when(crossed)
            def _():
                y_copy(0, idx).wait_recv()
                yr[idx] = yr[idx] + (ob[q] + rb[parity, q])

            @pl.when(jnp.logical_not(crossed))
            def _():
                yr[idx] = ob[q] + rb[parity, q]

            @pl.when((k >= place) & (place > 0))
            def _():
                z_copy(idx, idx, place).wait_recv()
                yr[idx] = yr[idx] + z[idx]

            @pl.when((k <= place) & (place < line - 1))
            def _():
                slot = jnp.where(k == place, line, k) * chunks + j
                z_copy(idx, slot, place).wait_recv()
                yr[idx] = yr[idx] + z[slot]

            @pl.when(k != place)
            def _():
                to = jnp.where(k > place, place + 1, place - 1)
                slot = jnp.where(k == place - 1, line, k) * chunks + j
                z_copy(idx, slot, to).start()

            @pl.when(k == place)
            def _():
                for o in range(1, owners):
                    x_copy(o, j).start()
                value = yr[idx]
                sq[...] += jnp.sum((value * value).reshape(rows // 8, 8, wide), axis=0)
                g[mp * chunks + j] = yr[idx, pl.ds(pl.multiple_of(mp * part, part), part)]

    @pl.loop(0, plan.ticks)
    def _(t):
        parity = lax.rem(t, 2)
        phase, step = t // half, lax.rem(t, half)
        crossing = t < plan.crossings
        y_k = mirrored(pick([[k for k, _ in row] for row in plan.order], at, phase))
        y_j = pick([[h for _, h in row] for row in plan.order], at, phase) * half + step
        deferring = t < half
        ahead = plan.lag + jnp.where(at == 0, 4, half + 2 + 2 * at)
        i = t - ahead
        forward = (i >= 0) & (i < (line - 1 - at) * chunks)
        ending = (t >= plan.last)
        i = jnp.maximum(i, 0)
        m_on = forward | (ending & (at > 0))
        m_k = mirrored(jnp.where(forward, line - 1 - i // chunks, at))
        m_j = jnp.where(forward, i % chunks, t - plan.last)
        n = t - (plan.lag + half + 2 + 2 * (line - 1 - at))
        backward = (at > 0) & (n >= 0) & (n < at * chunks)
        n = jnp.maximum(n, 0)
        s_on = backward | (ending & (at == 0))
        s_k = mirrored(jnp.where(backward, n // chunks, at))
        s_j = jnp.where(backward, n % chunks, t - plan.last)

        produce(0, crossing, y_k, 1 - lane, y_j, step == 0, parity)
        produce(1, deferring, beside, 1 - lane, t, t == 0, parity)
        produce(2, m_on, m_k, lane, m_j, m_j == 0, parity)
        produce(3, s_on, s_k, lane, s_j, s_j == 0, parity)

        slot = lax.rem(t, RING)
        y_idx = y_k * chunks + y_j

        @pl.when(crossing)
        def _():
            @pl.when(t >= RING)
            def _():
                y_copy(slot, 0).wait_send()

            core_copy(0, parity).wait()
            w[slot] = ob[0] + rb[parity, 0]

            @pl.when((y_k == place) & (y_j < half))
            def _():
                d_copy(y_j).wait_recv()
                w[slot] = w[slot] + dr[y_j]

            y_copy(slot, y_idx).start()

        @pl.when(deferring)
        def _():
            core_copy(1, parity).wait()
            ds[t] = ob[1] + rb[parity, 1]
            d_copy(t).start()

        own(2, m_on, m_k, m_j, parity)
        own(3, s_on, s_k, s_j, parity)

    total = sq[:, pl.ds(0, 128)]
    for i in range(1, wide // 128):
        total = total + sq[:, pl.ds(i * 128, 128)]
    parts[0] = total

    @pl.loop(1, devices)
    def _(o):
        part_copy(o).start()

    @pl.loop(0, chunks)
    def _(j):
        out_copy(mp * chunks + j).start()

    for o in range(1, owners):
        @pl.loop(0, chunks)
        def _(j):
            i = lax.rem(mp + o, owners) * chunks + j
            pltpu.make_async_remote_copy(
                g.at[i], g.at[i], x_send.at[0], x_recv.at[i], device_id=(dp, mp), device_id_type=MESH
            ).wait_recv()
            out_copy(i).start()

    others = parts.at[pl.ds(1, devices - 1)]
    everyone = pltpu.make_async_remote_copy(others, others, p_send, p_recv, device_id=(dp, mp), device_id_type=MESH)
    everyone.wait_recv()
    total_ref[...] = jnp.full(total_ref.shape, jnp.sum(jnp.sum(parts[...], axis=0)))
    everyone.wait_send()

    @pl.loop(0, owners * chunks)
    def _(i):
        out_copy(i).wait()

    @pl.loop(0, half)
    def _(j):
        d_copy(j).wait_send()

    @pl.loop(0, RING)
    def _(slot):
        y_copy(slot, 0).wait_send()

    @pl.loop(0, line * chunks)
    def _(i):
        @pl.when(i // chunks != place)
        def _():
            z_copy(i, 0, place).wait_send()

    for o in range(1, owners):
        @pl.loop(0, chunks)
        def _(j):
            x_copy(o, j).wait_send()


def reduced_gradient(plan, ff_blocks, layer_active, rows_in, rows_ct):
    rows, wide, chunks, line, half = plan.rows, plan.wide, plan.chunks, plan.line, plan.half
    devices = plan.replicas * plan.owners
    f32, dma = jnp.float32, pltpu.SemaphoreType.DMA

    def held(*lead):
        return pltpu.VMEM((*lead, rows, wide), f32)

    return pl.pallas_call(
        functools.partial(kernel, plan),
        out_shape=(
            jax.ShapeDtypeStruct((plan.part, plan.owners * plan.cols), f32),
            jax.ShapeDtypeStruct((8, 128), f32),
        ),
        in_specs=[
            pl.BlockSpec(memory_space=pltpu.SMEM),
            pl.BlockSpec(memory_space=pltpu.SMEM),
            pl.BlockSpec(memory_space=pl.ANY),
            pl.BlockSpec(memory_space=pl.ANY),
        ],
        out_specs=(pl.BlockSpec(memory_space=pl.ANY), pl.BlockSpec(memory_space=pltpu.VMEM)),
        scratch_shapes=[
            pltpu.VMEM((plan.tokens, plan.width), jnp.bfloat16),
            pltpu.VMEM((plan.tokens, plan.cols), jnp.bfloat16),
            pltpu.VMEM((4, 2, rows, plan.tokens), jnp.bfloat16),
            held(RING),
            held(line * chunks),
            held((line + 1) * chunks),
            held(half),
            held(half),
            held(4),
            held(2, 4),
            held(4),
            pltpu.VMEM((plan.owners * chunks, plan.part, wide), f32),
            pltpu.VMEM((8, wide), f32),
            pltpu.VMEM((devices, 8, 128), f32),
            dma((2,)),
            dma((4,)),
            dma((2, 4)),
            dma((RING,)),
            dma((line * chunks,)),
            dma((line * chunks,)),
            dma(((line + 1) * chunks,)),
            dma((half,)),
            dma((half,)),
            dma((max(1, plan.owners - 1) * chunks,)),
            dma((plan.owners * chunks,)),
            dma((plan.owners * chunks,)),
            dma,
            dma,
        ],
        compiler_params=pltpu.CompilerParams(collective_id=0, has_side_effects=True, vmem_limit_bytes=67043328),
        cost_estimate=pl.CostEstimate(
            flops=2 * plan.tokens * plan.width * plan.cols, bytes_accessed=32 << 20, transcendentals=0
        ),
        name="reduced_gradient",
    )(ff_blocks, layer_active, rows_in, rows_ct)


def shards(inputs, gate_cotangent, ff_blocks, layer_active, param, moment, second_moment):
    subnets, tokens, width = inputs.shape
    local_cols = gate_cotangent.shape[2]
    replicas, owners = lax.axis_size("dp"), lax.axis_size("mp")
    plan = Plan(replicas, owners, width, local_cols, subnets * tokens)
    gradient, total_sq = reduced_gradient(
        plan,
        ff_blocks,
        layer_active,
        inputs.reshape(subnets * tokens, width),
        gate_cotangent.reshape(subnets * tokens, local_cols),
    )
    total = jnp.sqrt(total_sq[0, 0])
    factor = jnp.minimum(1.0, math.sqrt(1.0 * width * local_cols * owners) / (total + 1e-06))
    clipped = gradient * factor
    new_moment = 0.9 * moment + 0.1 * clipped
    new_second = 0.95 * second_moment + 0.05 * clipped * clipped
    first_hat = new_moment / (1.0 - 0.9**STEP)
    second_hat = new_second / (1.0 - 0.95**STEP)
    new_param = param - 0.02 * (first_hat / (jnp.sqrt(second_hat) + 1e-08) + 0.1 * param)
    return (new_param, new_moment, new_second)


def solution(mesh):
    in_specs = (
        P(None, "dp", None),
        P(None, "dp", "mp"),
        P(),
        P(),
        P(("dp", "mp"), None),
        P(("dp", "mp"), None),
        P(("dp", "mp"), None),
    )
    out_specs = (P(("dp", "mp"), None), P(("dp", "mp"), None), P(("dp", "mp"), None))
    return jax.shard_map(shards, mesh=mesh, in_specs=in_specs, out_specs=out_specs, check_vma=False)
```

```python
import functools
import math

import jax
import jax.numpy as jnp
from jax import lax
from jax.experimental import pallas as pl
from jax.experimental.pallas import tpu as pltpu
from jax.sharding import PartitionSpec as P

BLOCK = 128
STEP = 10
MESH = pl.DeviceIdType.MESH
RING = 4


class Plan:
    def __init__(self, replicas, owners, width, local_cols, tokens):
        self.replicas, self.owners, self.tokens = replicas, owners, tokens
        self.line = line = replicas // 4
        self.rows = width // replicas
        self.part = self.rows // owners
        self.width, self.cols = width, local_cols
        self.wide = wide = 256 if local_cols % 512 == 0 else 128
        self.chunks = chunks = local_cols // wide
        self.half = half = chunks // 2
        self.crossings = line * chunks - half
        self.lag = 0
        while not self.fits():
            self.lag += 1
            assert self.lag < 1000
        self.ticks = self.last + chunks

    def fits(self):
        line, chunks, half = self.line, self.chunks, self.half
        self.last = (line - 1) * chunks - half + 4 + self.lag
        self.order = []
        good = True
        for at in range(line // 2):
            need = []
            for k in range(line):
                for h in range(2):
                    if (k, h) != (at ^ 1, 0):
                        need.append((self.tick_of(at, k, h * half), k, h))
            self.order.append([(k, h) for _, k, h in sorted(need)])
            for p, (k, h) in enumerate(self.order[-1]):
                for i in range(half):
                    good &= p * half + i <= self.tick_of(at, k, h * half + i)
                    good &= k != at or h == 1 or p * half + i > i
            good &= self.order[-1][0][1] == 0
            good &= at == 0 or self.tick_of(at, at + 1, chunks - 1) < self.last
            good &= at == 0 or self.tick_of(at, at - 1, chunks - 1) < self.last
        return good

    def start(self, distance):
        return self.lag + (self.half + 2 + 2 * distance if distance else 4)

    def tick_of(self, at, k, j):
        if k == at:
            return self.last + j
        if k > at:
            return self.start(at) + (self.line - 1 - k) * self.chunks + j
        return self.start(self.line - 1 - at) + k * self.chunks + j


def pick(table, at, p):
    value = jnp.int32(0)
    for a, row in enumerate(table):
        for q, entry in enumerate(row):
            if entry:
                value = jnp.where((at == a) & (p == q), jnp.int32(entry), value)
    return value


def kernel(plan, limit, x_hbm, c_hbm, g_hbm, total_ref, x, c, xt, w, yr, z, dr, sb, rb, ob, sq, parts,
           x_load, c_load, d2d_send, d2d_recv, y_send, y_recv, z_send, z_recv, d_send, d_recv, x_send, x_recv, keep_sem,
           p_send, p_recv):
    line, chunks, half, rows, wide = plan.line, plan.chunks, plan.half, plan.rows, plan.wide
    owners, part = plan.owners, plan.part
    dp, mp = lax.axis_index("dp"), lax.axis_index("mp")
    devices = plan.replicas * owners
    me = dp * owners + mp
    place, lane, core = dp // 4, (dp // 2) % 2, dp % 2
    other_core, other_lane = dp + 1 - 2 * core, dp + 2 - 4 * lane
    beside = place + 1 - 2 * (place % 2)
    far = place >= line // 2
    at = jnp.where(far, line - 1 - place, place)

    def mirrored(k):
        return jnp.where(far, line - 1 - k, k)

    def x_in(k, to_lane):
        block = k * 2 + to_lane
        cols = pl.ds(pl.multiple_of(block * 2 * rows, 2 * rows), 2 * rows)
        return pltpu.make_async_copy(x_hbm.at[:, cols], x.at[:, cols], x_load.at[block])

    def c_in(j):
        cols = pl.ds(pl.multiple_of(j * wide, wide), wide)
        return pltpu.make_async_copy(c_hbm.at[:, cols], c.at[:, cols], c_load.at[j])

    opening = mirrored(pick([[row[0][0]] for row in plan.order], at, 0))
    x_in(opening, 1 - lane).start()
    c_in(0).start()
    x_in(beside, 1 - lane).start()
    barrier = pltpu.get_barrier_semaphore()

    @pl.loop(1, devices)
    def _(o):
        other = lax.rem(me + o, devices)
        pl.semaphore_signal(barrier, inc=1, device_id=(other // owners, other % owners), device_id_type=MESH)

    def load_rest():
        @pl.loop(1, chunks)
        def _(j):
            c_in(j).start()

        @pl.loop(0, line)
        def _(k):
            @pl.when((k != opening) & (k != beside))
            def _():
                x_in(k, 1 - lane).start()

            x_in(k, lane).start()

    first_block = mp * (plan.cols // BLOCK)
    subnets = limit.shape[0]
    tokens = plan.tokens // subnets

    def ready(j):
        c_in(j).wait()
        for i in range(wide // BLOCK):
            b = j * (wide // BLOCK) + i
            cols = pl.ds(pl.multiple_of(b * BLOCK, BLOCK), BLOCK)
            for s in range(subnets):
                keep = first_block + b < limit[s]
                spot = (pl.ds(s * tokens, tokens), cols)
                c[spot] = jnp.where(keep, c[spot], jnp.zeros((), c.dtype))

    sq[...] = jnp.zeros_like(sq)

    def core_copy(q, parity):
        return pltpu.make_async_remote_copy(
            sb.at[q], rb.at[parity, q], d2d_send.at[q], d2d_recv.at[parity, q], device_id=(other_core, mp), device_id_type=MESH
        )

    def y_copy(slot, idx):
        return pltpu.make_async_remote_copy(
            w.at[slot], yr.at[idx], y_send.at[slot], y_recv.at[idx], device_id=(other_lane, mp), device_id_type=MESH
        )

    def d_copy(j):
        return pltpu.make_async_remote_copy(
            yr.at[beside * chunks + j], dr.at[j], d_send.at[j], d_recv.at[j], device_id=(dp + 4 * (beside - place), mp), device_id_type=MESH
        )

    def z_copy(idx, slot, to):
        return pltpu.make_async_remote_copy(
            yr.at[idx], z.at[slot], z_send.at[idx], z_recv.at[slot], device_id=(dp + 4 * (to - place), mp), device_id_type=MESH
        )

    def result(i):
        return g_hbm.at[:, pl.ds(pl.multiple_of(i * wide, wide), wide)]

    def x_copy(o, j):
        to = lax.rem(mp + o, owners)
        spot = yr.at[place * chunks + j, pl.ds(pl.multiple_of(to * part, part), part)]
        return pltpu.make_async_remote_copy(
            spot, result(mp * chunks + j), x_send.at[(o - 1) * chunks + j], x_recv.at[mp * chunks + j],
            device_id=(dp, to), device_id_type=MESH,
        )

    def keep_copy(j):
        spot = yr.at[place * chunks + j, pl.ds(pl.multiple_of(mp * part, part), part)]
        return pltpu.make_async_copy(spot, result(mp * chunks + j), keep_sem.at[j])

    def part_copy(o):
        other = lax.rem(me + o, devices)
        return pltpu.make_async_remote_copy(
            parts.at[0, pl.ds(0, 1)], parts.at[devices - o, pl.ds(0, 1)], p_send, p_recv,
            device_id=(other // owners, other % owners), device_id_type=MESH,
        )

    def produce(q, on, k, to_lane, j, fresh, first_use, parity, first_tick=None):
        @pl.when(on)
        def _():
            @pl.when(first_use)
            def _():
                x_in(k, to_lane).wait()

            @pl.when(fresh)
            def _():
                for side, owner in enumerate((1 - core, core)):
                    first = pl.multiple_of(((k * 2 + to_lane) * 2 + owner) * rows, rows)
                    xt[q, side] = x[:, pl.ds(first, rows)].T

            cols = pl.ds(pl.multiple_of(j * wide, wide), wide)
            sb[q] = jnp.dot(xt[q, 0], c[:, cols], preferred_element_type=jnp.float32)
            ob[q] = jnp.dot(xt[q, 1], c[:, cols], preferred_element_type=jnp.float32)

            if q == 0:
                @pl.when(first_tick)
                def _():
                    pl.semaphore_wait(barrier, devices - 1)

            core_copy(q, parity).start()

    def own(q, on, k, j, parity):
        idx = k * chunks + j

        @pl.when(on)
        def _():
            core_copy(q, parity).wait()
            crossed = (k != beside) | (j >= half)

            @pl.when(crossed)
            def _():
                y_copy(0, idx).wait_recv()
                yr[idx] = yr[idx] + (ob[q] + rb[parity, q])

            @pl.when(jnp.logical_not(crossed))
            def _():
                d_copy(j).wait_send()
                yr[idx] = ob[q] + rb[parity, q]

            @pl.when((k >= place) & (place > 0))
            def _():
                z_copy(idx, idx, place).wait_recv()
                yr[idx] = yr[idx] + z[idx]

            @pl.when((k <= place) & (place < line - 1))
            def _():
                slot = jnp.where(k == place, line, k) * chunks + j
                z_copy(idx, slot, place).wait_recv()
                yr[idx] = yr[idx] + z[slot]

            @pl.when(k != place)
            def _():
                to = jnp.where(k > place, place + 1, place - 1)
                slot = jnp.where(k == place - 1, line, k) * chunks + j
                z_copy(idx, slot, to).start()

            @pl.when(k == place)
            def _():
                for o in range(1, owners):
                    x_copy(o, j).start()
                value = yr[idx]
                sq[...] += jnp.sum((value * value).reshape(rows // 8, 8, wide), axis=0)
                keep_copy(j).start()

    @pl.loop(0, plan.ticks)
    def _(t):
        parity = lax.rem(t, 2)
        phase, step = t // half, lax.rem(t, half)
        crossing = t < plan.crossings
        y_k = mirrored(pick([[k for k, _ in row] for row in plan.order], at, phase))
        y_j = pick([[h for _, h in row] for row in plan.order], at, phase) * half + step
        deferring = t < half
        ahead = plan.lag + jnp.where(at == 0, 4, half + 2 + 2 * at)
        i = t - ahead
        forward = (i >= 0) & (i < (line - 1 - at) * chunks)
        ending = (t >= plan.last)
        i = jnp.maximum(i, 0)
        m_on = forward | (ending & (at > 0))
        m_k = mirrored(jnp.where(forward, line - 1 - i // chunks, at))
        m_j = jnp.where(forward, i % chunks, t - plan.last)
        n = t - (plan.lag + half + 2 + 2 * (line - 1 - at))
        backward = (at > 0) & (n >= 0) & (n < at * chunks)
        n = jnp.maximum(n, 0)
        s_on = backward | (ending & (at == 0))
        s_k = mirrored(jnp.where(backward, n // chunks, at))
        s_j = jnp.where(backward, n % chunks, t - plan.last)

        @pl.when(t < chunks)
        def _():
            ready(t)

        third_k = jnp.where(deferring, beside, s_k)
        third_j = jnp.where(deferring, t, s_j)
        third_lane = jnp.where(deferring, 1 - lane, lane)
        produce(0, crossing, y_k, 1 - lane, y_j, step == 0, (y_j == 0) & (y_k != beside), parity, t == 0)

        @pl.when(t == 0)
        def _():
            load_rest()

        produce(1, m_on, m_k, lane, m_j, m_j == 0, m_j == 0, parity)
        produce(2, deferring | s_on, third_k, third_lane, third_j, third_j == 0, third_j == 0, parity)

        slot = lax.rem(t, RING)
        y_idx = y_k * chunks + y_j

        @pl.when(crossing)
        def _():
            @pl.when(t >= RING)
            def _():
                y_copy(slot, 0).wait_send()

            core_copy(0, parity).wait()
            w[slot] = ob[0] + rb[parity, 0]

            @pl.when((y_k == place) & (y_j < half))
            def _():
                d_copy(y_j).wait_recv()
                w[slot] = w[slot] + dr[y_j]

            y_copy(slot, y_idx).start()

        @pl.when(deferring)
        def _():
            core_copy(2, parity).wait()
            yr[beside * chunks + t] = ob[2] + rb[parity, 2]
            d_copy(t).start()

        own(1, m_on, m_k, m_j, parity)
        own(2, s_on, s_k, s_j, parity)

    total = sq[:, pl.ds(0, 128)]
    for i in range(1, wide // 128):
        total = total + sq[:, pl.ds(i * 128, 128)]
    parts[0, pl.ds(0, 1)] = jnp.sum(total, axis=0, keepdims=True)

    @pl.loop(1, devices)
    def _(o):
        part_copy(o).start()

    @pl.loop(0, RING)
    def _(slot):
        y_copy(slot, 0).wait_send()

    @pl.loop(0, line * chunks)
    def _(i):
        @pl.when(i // chunks != place)
        def _():
            z_copy(i, 0, place).wait_send()

    @pl.loop(0, chunks)
    def _(j):
        keep_copy(j).wait()

    for o in range(1, owners):
        @pl.loop(0, chunks)
        def _(j):
            x_copy(o, j).wait_send()
            i = lax.rem(mp + o, owners) * chunks + j
            pltpu.make_async_remote_copy(
                result(i), result(i), x_send.at[0], x_recv.at[i], device_id=(dp, mp), device_id_type=MESH
            ).wait_recv()

    everyone = parts.at[pl.ds(1, devices - 1), pl.ds(0, 1)]
    arrivals = pltpu.make_async_remote_copy(everyone, everyone, p_send, p_recv, device_id=(dp, mp), device_id_type=MESH)
    arrivals.wait()
    total_ref[0, 0] = jnp.sum(jnp.sum(parts[:, pl.ds(0, 1), :], axis=0))


def reduced_gradient(plan, limit, rows_in, rows_ct):
    rows, wide, chunks, line, half = plan.rows, plan.wide, plan.chunks, plan.line, plan.half
    devices = plan.replicas * plan.owners
    f32, dma = jnp.float32, pltpu.SemaphoreType.DMA

    def held(*lead):
        return pltpu.VMEM((*lead, rows, wide), f32)

    buffers = [
        pltpu.VMEM((plan.tokens, plan.width), jnp.bfloat16),
        pltpu.VMEM((plan.tokens, plan.cols), jnp.bfloat16),
        pltpu.VMEM((3, 2, rows, plan.tokens), jnp.bfloat16),
        held(RING),
        held(line * chunks),
        held((line + 1) * chunks),
        held(half),
        held(3),
        held(2, 3),
        held(3),
        pltpu.VMEM((8, wide), f32),
        pltpu.VMEM((devices, 8, 128), f32),
    ]
    room = sum(math.prod(b.shape) * jnp.dtype(b.dtype).itemsize for b in buffers)
    return pl.pallas_call(
        functools.partial(kernel, plan),
        out_shape=(
            jax.ShapeDtypeStruct((plan.part, plan.owners * plan.cols), f32),
            jax.ShapeDtypeStruct((1, 1), f32),
        ),
        in_specs=[
            pl.BlockSpec(memory_space=pltpu.SMEM),
            pl.BlockSpec(memory_space=pl.ANY),
            pl.BlockSpec(memory_space=pl.ANY),
        ],
        out_specs=(pl.BlockSpec(memory_space=pl.ANY), pl.BlockSpec(memory_space=pltpu.SMEM)),
        scratch_shapes=[
            *buffers,
            dma((line * 2,)),
            dma((chunks,)),
            dma((3,)),
            dma((2, 3)),
            dma((RING,)),
            dma((line * chunks,)),
            dma((line * chunks,)),
            dma(((line + 1) * chunks,)),
            dma((half,)),
            dma((half,)),
            dma((max(1, plan.owners - 1) * chunks,)),
            dma((plan.owners * chunks,)),
            dma((chunks,)),
            dma,
            dma,
        ],
        compiler_params=pltpu.CompilerParams(collective_id=0, has_side_effects=True, vmem_limit_bytes=room + (1 << 20)),
        cost_estimate=pl.CostEstimate(
            flops=2 * plan.tokens * plan.width * plan.cols, bytes_accessed=32 << 20, transcendentals=0
        ),
        name="reduced_gradient",
    )(limit, rows_in, rows_ct)


def shards(inputs, gate_cotangent, ff_blocks, layer_active, param, moment, second_moment):
    subnets, tokens, width = inputs.shape
    local_cols = gate_cotangent.shape[2]
    replicas, owners = lax.axis_size("dp"), lax.axis_size("mp")
    plan = Plan(replicas, owners, width, local_cols, subnets * tokens)
    gradient, total_sq = reduced_gradient(
        plan,
        jnp.where(layer_active == 1, ff_blocks, 0),
        inputs.reshape(subnets * tokens, width),
        gate_cotangent.reshape(subnets * tokens, local_cols),
    )
    total = jnp.sqrt(total_sq[0, 0])
    factor = jnp.minimum(1.0, math.sqrt(1.0 * width * local_cols * owners) / (total + 1e-06))
    clipped = gradient * factor
    new_moment = 0.9 * moment + 0.1 * clipped
    new_second = 0.95 * second_moment + 0.05 * clipped * clipped
    first_hat = new_moment / (1.0 - 0.9**STEP)
    second_hat = new_second / (1.0 - 0.95**STEP)
    new_param = param - 0.02 * (first_hat / (jnp.sqrt(second_hat) + 1e-08) + 0.1 * param)
    return (new_param, new_moment, new_second)


def solution(mesh):
    in_specs = (
        P(None, "dp", None),
        P(None, "dp", "mp"),
        P(),
        P(),
        P(("dp", "mp"), None),
        P(("dp", "mp"), None),
        P(("dp", "mp"), None),
    )
    out_specs = (P(("dp", "mp"), None), P(("dp", "mp"), None), P(("dp", "mp"), None))
    return jax.shard_map(shards, mesh=mesh, in_specs=in_specs, out_specs=out_specs, check_vma=False)
```

```python
import functools
import math

import jax
import jax.numpy as jnp
from jax import lax
from jax.experimental import pallas as pl
from jax.experimental.pallas import tpu as pltpu
from jax.sharding import PartitionSpec as P

BLOCK = 128
STEP = 10
MESH = pl.DeviceIdType.MESH
RING = 4


class Plan:
    def __init__(self, replicas, owners, width, local_cols, tokens):
        self.replicas, self.owners, self.tokens = replicas, owners, tokens
        self.line = line = replicas // 4
        self.rows = width // replicas
        self.part = self.rows // owners
        self.width, self.cols = width, local_cols
        self.wide = wide = 256 if local_cols % 512 == 0 else 128
        self.chunks = chunks = local_cols // wide
        self.half = half = chunks // 2
        self.crossings = line * chunks - half
        self.lag = 0
        while not self.fits():
            self.lag += 1
            assert self.lag < 1000
        self.ticks = self.last + chunks

    def fits(self):
        line, chunks, half = self.line, self.chunks, self.half
        self.last = (line - 1) * chunks - half + 4 + self.lag
        self.order = []
        good = True
        for at in range(line // 2):
            need = []
            for k in range(line):
                for h in range(2):
                    if (k, h) != (at ^ 1, 0):
                        need.append((self.tick_of(at, k, h * half), k, h))
            self.order.append([(k, h) for _, k, h in sorted(need)])
            for p, (k, h) in enumerate(self.order[-1]):
                for i in range(half):
                    good &= p * half + i <= self.tick_of(at, k, h * half + i)
                    good &= k != at or h == 1 or p * half + i > i
            good &= self.order[-1][0][1] == 0
            good &= at == 0 or self.tick_of(at, at + 1, chunks - 1) < self.last
            good &= at == 0 or self.tick_of(at, at - 1, chunks - 1) < self.last
        return good

    def start(self, distance):
        return self.lag + (self.half + 2 + 2 * distance if distance else 4)

    def tick_of(self, at, k, j):
        if k == at:
            return self.last + j
        if k > at:
            return self.start(at) + (self.line - 1 - k) * self.chunks + j
        return self.start(self.line - 1 - at) + k * self.chunks + j


def pick(table, at, p):
    value = jnp.int32(0)
    for a, row in enumerate(table):
        for q, entry in enumerate(row):
            if entry:
                value = jnp.where((at == a) & (p == q), jnp.int32(entry), value)
    return value


def kernel(plan, limit, x_hbm, c_hbm, g_hbm, total_ref, x, c, xt, w, yr, z, dr, sb, rb, ob, sq, parts,
           x_load, c_load, d2d_send, d2d_recv, y_send, y_recv, z_send, z_recv, d_send, d_recv, x_send, x_recv, keep_sem,
           p_send, p_recv, y_tail, z_tail):
    line, chunks, half, rows, wide = plan.line, plan.chunks, plan.half, plan.rows, plan.wide
    owners, part = plan.owners, plan.part
    dp, mp = lax.axis_index("dp"), lax.axis_index("mp")
    devices = plan.replicas * owners
    me = dp * owners + mp
    place, lane, core = dp // 4, (dp // 2) % 2, dp % 2
    other_core, other_lane = dp + 1 - 2 * core, dp + 2 - 4 * lane
    beside = place + 1 - 2 * (place % 2)
    far = place >= line // 2
    at = jnp.where(far, line - 1 - place, place)

    def mirrored(k):
        return jnp.where(far, line - 1 - k, k)

    def x_in(k, to_lane):
        block = k * 2 + to_lane
        cols = pl.ds(pl.multiple_of(block * 2 * rows, 2 * rows), 2 * rows)
        return pltpu.make_async_copy(x_hbm.at[:, cols], x.at[:, cols], x_load.at[block])

    def c_in(j):
        cols = pl.ds(pl.multiple_of(j * wide, wide), wide)
        return pltpu.make_async_copy(c_hbm.at[:, cols], c.at[:, cols], c_load.at[j])

    opening = mirrored(pick([[row[0][0]] for row in plan.order], at, 0))
    x_in(opening, 1 - lane).start()
    c_in(0).start()
    x_in(beside, 1 - lane).start()
    barrier = pltpu.get_barrier_semaphore()

    @pl.loop(1, devices)
    def _(o):
        other = lax.rem(me + o, devices)
        pl.semaphore_signal(barrier, inc=1, device_id=(other // owners, other % owners), device_id_type=MESH)

    def load_rest():
        @pl.loop(1, chunks)
        def _(j):
            c_in(j).start()

        @pl.loop(0, line)
        def _(k):
            @pl.when((k != opening) & (k != beside))
            def _():
                x_in(k, 1 - lane).start()

            x_in(k, lane).start()

    first_block = mp * (plan.cols // BLOCK)
    subnets = limit.shape[0]
    tokens = plan.tokens // subnets

    def ready(j):
        c_in(j).wait()
        for i in range(wide // BLOCK):
            b = j * (wide // BLOCK) + i
            cols = pl.ds(pl.multiple_of(b * BLOCK, BLOCK), BLOCK)
            for s in range(subnets):
                keep = first_block + b < limit[s]
                spot = (pl.ds(s * tokens, tokens), cols)
                c[spot] = jnp.where(keep, c[spot], jnp.zeros((), c.dtype))

    sq[...] = jnp.zeros_like(sq)

    def core_copy(q, parity):
        return pltpu.make_async_remote_copy(
            sb.at[q], rb.at[parity, q], d2d_send.at[q], d2d_recv.at[parity, q], device_id=(other_core, mp), device_id_type=MESH
        )

    def y_copy(slot, idx):
        return pltpu.make_async_remote_copy(
            w.at[slot], yr.at[idx], y_send.at[slot], y_recv.at[idx], device_id=(other_lane, mp), device_id_type=MESH
        )

    def d_copy(j):
        return pltpu.make_async_remote_copy(
            yr.at[beside * chunks + j], dr.at[j], d_send.at[j], d_recv.at[j], device_id=(dp + 4 * (beside - place), mp), device_id_type=MESH
        )

    def z_copy(idx, slot, to):
        return pltpu.make_async_remote_copy(
            yr.at[idx], z.at[slot], z_send.at[idx], z_recv.at[slot], device_id=(dp + 4 * (to - place), mp), device_id_type=MESH
        )

    turns = [*range(1, owners), 0]

    def piece(o):
        return pl.ds(pl.multiple_of(lax.rem(mp + o, owners) * part, part), part)

    def y_piece(slot, idx, o):
        arrived = y_tail.at[(idx // chunks) * (owners - 1) + o - 1] if o else y_recv.at[idx]
        return pltpu.make_async_remote_copy(
            w.at[slot, piece(o)], yr.at[idx, piece(o)], y_send.at[slot], arrived,
            device_id=(other_lane, mp), device_id_type=MESH,
        )

    def z_piece(idx, slot, to, o):
        arrived = z_tail.at[(slot // chunks) * (owners - 1) + o - 1] if o else z_recv.at[slot]
        return pltpu.make_async_remote_copy(
            yr.at[idx, piece(o)], z.at[slot, piece(o)], z_send.at[idx], arrived,
            device_id=(dp + 4 * (to - place), mp), device_id_type=MESH,
        )

    def result(i):
        return g_hbm.at[:, pl.ds(pl.multiple_of(i * wide, wide), wide)]

    def x_copy(o, j):
        to = lax.rem(mp + o, owners)
        spot = yr.at[place * chunks + j, pl.ds(pl.multiple_of(to * part, part), part)]
        return pltpu.make_async_remote_copy(
            spot, result(mp * chunks + j), x_send.at[(o - 1) * chunks + j], x_recv.at[mp * chunks + j],
            device_id=(dp, to), device_id_type=MESH,
        )

    def keep_copy(j):
        spot = yr.at[place * chunks + j, pl.ds(pl.multiple_of(mp * part, part), part)]
        return pltpu.make_async_copy(spot, result(mp * chunks + j), keep_sem.at[j])

    def part_copy(o):
        other = lax.rem(me + o, devices)
        return pltpu.make_async_remote_copy(
            parts.at[0, pl.ds(0, 1)], parts.at[devices - o, pl.ds(0, 1)], p_send, p_recv,
            device_id=(other // owners, other % owners), device_id_type=MESH,
        )

    def produce(q, on, k, to_lane, j, fresh, first_use, parity, first_tick=None):
        @pl.when(on)
        def _():
            @pl.when(first_use)
            def _():
                x_in(k, to_lane).wait()

            @pl.when(fresh)
            def _():
                for side, owner in enumerate((1 - core, core)):
                    first = pl.multiple_of(((k * 2 + to_lane) * 2 + owner) * rows, rows)
                    xt[q, side] = x[:, pl.ds(first, rows)].T

            cols = pl.ds(pl.multiple_of(j * wide, wide), wide)
            sb[q] = jnp.dot(xt[q, 0], c[:, cols], preferred_element_type=jnp.float32)
            ob[q] = jnp.dot(xt[q, 1], c[:, cols], preferred_element_type=jnp.float32)

            if q == 0:
                @pl.when(first_tick)
                def _():
                    pl.semaphore_wait(barrier, devices - 1)

            core_copy(q, parity).start()

    def squares(value):
        sq[...] += jnp.sum((value * value).reshape(value.shape[0] // 8, 8, wide), axis=0)

    def own(q, on, k, j, parity):
        idx = k * chunks + j
        from_left = (k >= place) & (place > 0)
        from_right = (k <= place) & (place < line - 1)
        right_slot = jnp.where(k == place, line, k) * chunks + j
        to = jnp.where(k > place, place + 1, place - 1)
        to_slot = jnp.where(k == place - 1, line, k) * chunks + j

        def whole():
            crossed = (k != beside) | (j >= half)

            @pl.when(crossed)
            def _():
                y_copy(0, idx).wait_recv()
                yr[idx] = yr[idx] + (ob[q] + rb[parity, q])

            @pl.when(jnp.logical_not(crossed))
            def _():
                d_copy(j).wait_send()
                yr[idx] = ob[q] + rb[parity, q]

            @pl.when(from_left)
            def _():
                z_copy(idx, idx, place).wait_recv()
                yr[idx] = yr[idx] + z[idx]

            @pl.when(from_right)
            def _():
                z_copy(idx, right_slot, place).wait_recv()
                yr[idx] = yr[idx] + z[right_slot]

            @pl.when(k != place)
            def _():
                z_copy(idx, to_slot, to).start()

            @pl.when(k == place)
            def _():
                for o in range(1, owners):
                    x_copy(o, j).start()
                squares(yr[idx])
                keep_copy(j).start()

        def in_pieces(o):
            spot = piece(o)
            y_piece(0, idx, o).wait_recv()
            yr[idx, spot] = yr[idx, spot] + (ob[q, spot] + rb[parity, q, spot])

            @pl.when(from_left)
            def _():
                z_piece(idx, idx, place, o).wait_recv()
                yr[idx, spot] = yr[idx, spot] + z[idx, spot]

            @pl.when(from_right)
            def _():
                z_piece(idx, right_slot, place, o).wait_recv()
                yr[idx, spot] = yr[idx, spot] + z[right_slot, spot]

            @pl.when(k != place)
            def _():
                z_piece(idx, to_slot, to, o).start()

            @pl.when(k == place)
            def _():
                if o:
                    x_copy(o, j).start()
                squares(yr[idx, spot])
                if not o:
                    keep_copy(j).start()

        @pl.when(on)
        def _():
            core_copy(q, parity).wait()

            @pl.when(j < chunks - 1)
            def _():
                whole()

            @pl.when(j == chunks - 1)
            def _():
                for o in turns:
                    in_pieces(o)

    @pl.loop(0, plan.ticks)
    def _(t):
        parity = lax.rem(t, 2)
        phase, step = t // half, lax.rem(t, half)
        crossing = t < plan.crossings
        y_k = mirrored(pick([[k for k, _ in row] for row in plan.order], at, phase))
        y_j = pick([[h for _, h in row] for row in plan.order], at, phase) * half + step
        deferring = t < half
        ahead = plan.lag + jnp.where(at == 0, 4, half + 2 + 2 * at)
        i = t - ahead
        forward = (i >= 0) & (i < (line - 1 - at) * chunks)
        ending = (t >= plan.last)
        i = jnp.maximum(i, 0)
        m_on = forward | (ending & (at > 0))
        m_k = mirrored(jnp.where(forward, line - 1 - i // chunks, at))
        m_j = jnp.where(forward, i % chunks, t - plan.last)
        n = t - (plan.lag + half + 2 + 2 * (line - 1 - at))
        backward = (at > 0) & (n >= 0) & (n < at * chunks)
        n = jnp.maximum(n, 0)
        s_on = backward | (ending & (at == 0))
        s_k = mirrored(jnp.where(backward, n // chunks, at))
        s_j = jnp.where(backward, n % chunks, t - plan.last)

        @pl.when(t < chunks)
        def _():
            ready(t)

        third_k = jnp.where(deferring, beside, s_k)
        third_j = jnp.where(deferring, t, s_j)
        third_lane = jnp.where(deferring, 1 - lane, lane)
        produce(0, crossing, y_k, 1 - lane, y_j, step == 0, (y_j == 0) & (y_k != beside), parity, t == 0)

        @pl.when(t == 0)
        def _():
            load_rest()

        produce(1, m_on, m_k, lane, m_j, m_j == 0, m_j == 0, parity)
        produce(2, deferring | s_on, third_k, third_lane, third_j, third_j == 0, third_j == 0, parity)

        slot = lax.rem(t, RING)
        y_idx = y_k * chunks + y_j

        @pl.when(crossing)
        def _():
            @pl.when(t >= RING)
            def _():
                y_copy(slot, 0).wait_send()

            core_copy(0, parity).wait()
            w[slot] = ob[0] + rb[parity, 0]

            @pl.when((y_k == place) & (y_j < half))
            def _():
                d_copy(y_j).wait_recv()
                w[slot] = w[slot] + dr[y_j]

            @pl.when(y_j < chunks - 1)
            def _():
                y_copy(slot, y_idx).start()

            @pl.when(y_j == chunks - 1)
            def _():
                for o in turns:
                    y_piece(slot, y_idx, o).start()

        @pl.when(deferring)
        def _():
            core_copy(2, parity).wait()
            yr[beside * chunks + t] = ob[2] + rb[parity, 2]
            d_copy(t).start()

        own(1, m_on, m_k, m_j, parity)
        own(2, s_on, s_k, s_j, parity)

    total = sq[:, pl.ds(0, 128)]
    for i in range(1, wide // 128):
        total = total + sq[:, pl.ds(i * 128, 128)]
    parts[0, pl.ds(0, 1)] = jnp.sum(total, axis=0, keepdims=True)

    @pl.loop(1, devices)
    def _(o):
        part_copy(o).start()

    @pl.loop(0, RING)
    def _(slot):
        y_copy(slot, 0).wait_send()

    @pl.loop(0, line * chunks)
    def _(i):
        @pl.when(i // chunks != place)
        def _():
            z_copy(i, 0, place).wait_send()

    @pl.loop(0, chunks)
    def _(j):
        keep_copy(j).wait()

    for o in range(1, owners):
        @pl.loop(0, chunks)
        def _(j):
            x_copy(o, j).wait_send()
            i = lax.rem(mp + o, owners) * chunks + j
            pltpu.make_async_remote_copy(
                result(i), result(i), x_send.at[0], x_recv.at[i], device_id=(dp, mp), device_id_type=MESH
            ).wait_recv()

    everyone = parts.at[pl.ds(1, devices - 1), pl.ds(0, 1)]
    arrivals = pltpu.make_async_remote_copy(everyone, everyone, p_send, p_recv, device_id=(dp, mp), device_id_type=MESH)
    arrivals.wait()
    total_ref[0, 0] = jnp.sum(jnp.sum(parts[:, pl.ds(0, 1), :], axis=0))


def reduced_gradient(plan, limit, rows_in, rows_ct):
    rows, wide, chunks, line, half = plan.rows, plan.wide, plan.chunks, plan.line, plan.half
    devices = plan.replicas * plan.owners
    f32, dma = jnp.float32, pltpu.SemaphoreType.DMA

    def held(*lead):
        return pltpu.VMEM((*lead, rows, wide), f32)

    buffers = [
        pltpu.VMEM((plan.tokens, plan.width), jnp.bfloat16),
        pltpu.VMEM((plan.tokens, plan.cols), jnp.bfloat16),
        pltpu.VMEM((3, 2, rows, plan.tokens), jnp.bfloat16),
        held(RING),
        held(line * chunks),
        held((line + 1) * chunks),
        held(half),
        held(3),
        held(2, 3),
        held(3),
        pltpu.VMEM((8, wide), f32),
        pltpu.VMEM((devices, 8, 128), f32),
    ]
    room = sum(math.prod(b.shape) * jnp.dtype(b.dtype).itemsize for b in buffers)
    return pl.pallas_call(
        functools.partial(kernel, plan),
        out_shape=(
            jax.ShapeDtypeStruct((plan.part, plan.owners * plan.cols), f32),
            jax.ShapeDtypeStruct((1, 1), f32),
        ),
        in_specs=[
            pl.BlockSpec(memory_space=pltpu.SMEM),
            pl.BlockSpec(memory_space=pl.ANY),
            pl.BlockSpec(memory_space=pl.ANY),
        ],
        out_specs=(pl.BlockSpec(memory_space=pl.ANY), pl.BlockSpec(memory_space=pltpu.SMEM)),
        scratch_shapes=[
            *buffers,
            dma((line * 2,)),
            dma((chunks,)),
            dma((3,)),
            dma((2, 3)),
            dma((RING,)),
            dma((line * chunks,)),
            dma((line * chunks,)),
            dma(((line + 1) * chunks,)),
            dma((half,)),
            dma((half,)),
            dma((max(1, plan.owners - 1) * chunks,)),
            dma((plan.owners * chunks,)),
            dma((chunks,)),
            dma,
            dma,
            dma((line * max(1, plan.owners - 1),)),
            dma(((line + 1) * max(1, plan.owners - 1),)),
        ],
        compiler_params=pltpu.CompilerParams(collective_id=0, has_side_effects=True, vmem_limit_bytes=room + (1 << 20)),
        cost_estimate=pl.CostEstimate(
            flops=2 * plan.tokens * plan.width * plan.cols, bytes_accessed=32 << 20, transcendentals=0
        ),
        name="reduced_gradient",
    )(limit, rows_in, rows_ct)


def shards(inputs, gate_cotangent, ff_blocks, layer_active, param, moment, second_moment):
    subnets, tokens, width = inputs.shape
    local_cols = gate_cotangent.shape[2]
    replicas, owners = lax.axis_size("dp"), lax.axis_size("mp")
    plan = Plan(replicas, owners, width, local_cols, subnets * tokens)
    gradient, total_sq = reduced_gradient(
        plan,
        jnp.where(layer_active == 1, ff_blocks, 0),
        inputs.reshape(subnets * tokens, width),
        gate_cotangent.reshape(subnets * tokens, local_cols),
    )
    total = jnp.sqrt(total_sq[0, 0])
    factor = jnp.minimum(1.0, math.sqrt(1.0 * width * local_cols * owners) / (total + 1e-06))
    clipped = gradient * factor
    new_moment = 0.9 * moment + 0.1 * clipped
    new_second = 0.95 * second_moment + 0.05 * clipped * clipped
    first_hat = new_moment / (1.0 - 0.9**STEP)
    second_hat = new_second / (1.0 - 0.95**STEP)
    new_param = param - 0.02 * (first_hat / (jnp.sqrt(second_hat) + 1e-08) + 0.1 * param)
    return (new_param, new_moment, new_second)


def solution(mesh):
    in_specs = (
        P(None, "dp", None),
        P(None, "dp", "mp"),
        P(),
        P(),
        P(("dp", "mp"), None),
        P(("dp", "mp"), None),
        P(("dp", "mp"), None),
    )
    out_specs = (P(("dp", "mp"), None), P(("dp", "mp"), None), P(("dp", "mp"), None))
    return jax.shard_map(shards, mesh=mesh, in_specs=in_specs, out_specs=out_specs, check_vma=False)
```
